32 devices in a mesh: chan: 4 (over x, core), az: 8 (over z, y).
Axes of the slice: x: 2, y: 2, z: 4, core: 2. Of those that a mesh axis runs over, the one named last changes fastest.
Arguments:
- signal: bfloat16 [4, 2, 128, 8192], P('chan', None, 'az'), may hold values from -6 to 6
- tap_table: float32 [64, 16], replicated, may hold values from -1.5 to 1.5
- range_shift: int32 [1024], P('az'), may hold values from -8 to 8
- tap_index: int32 [1024], P('az'), may hold values from 0 to 63
- ref_channel: int32 [8], P('az'), may hold values from 0 to 3
Outputs:
- picture: float32 [4, 2, 128, 1024], P('chan', None, None, 'az')
The draws below stay inside these ranges and needn't reach their ends.
All inputs are finite; a program needn't handle non-finite values.
Results may differ from the reference program's by a relative error of at most 0.012.
Values may be sent and summed in bfloat16 or wider, within the bound.
A program may use at most 64 MiB of HBM per device.

```python
import math
import jax
import jax.numpy as jnp
from jax import lax

TAPS = 16
MAXSHIFT = 8
NTAB = 64
GUARD = 16
CHAN = 4
PULSES = 128
NR = 8192
R = 1024
HALO = 16
N_AZ = 8


def touch_ends(array, rng, low, top_value):
    dims = array.shape
    index_at = [jax.random.randint(jax.random.fold_in(rng, axis), (), 0, dims[axis]) for axis in range(len(dims))]
    array = array.at[tuple(index_at)].set(low)
    longest = dims.index(max(dims))
    index_at[longest] = (index_at[longest] + 1) % dims[longest]
    return array.at[tuple(index_at)].set(top_value)


def levels(rng, dims, cuts, low, largest):
    def one(position, parts):
        heights = jax.random.uniform(jax.random.fold_in(jax.random.fold_in(rng, 6), position), (parts,), jnp.float32, low / len(cuts), largest / len(cuts))
        return jnp.repeat(jnp.exp(heights), dims[position] // parts).reshape((-1,) + (1,) * (len(dims) - position - 1))

    loudness = one(*cuts[0])
    for cut in cuts[1:]:
        loudness = loudness * one(*cut)
    return loudness


def scatter_about(key, dims, spread, most, cuts=(), kind=jnp.bfloat16):
    entries = spread * jax.random.normal(key, dims, jnp.float32)
    if cuts:
        entries = entries * levels(key, dims, cuts, -0.22, 0.18)
    return jnp.clip(entries, -most, most).astype(kind)


def setup_inputs(seed: int = 0) -> dict:
    key_list = jax.random.split(jax.random.key(seed), 6)
    signal = scatter_about(key_list[0], (CHAN, 2, PULSES, NR), 1.0, 6.0, ((0, 4), (2, 8)))
    tap_table = scatter_about(key_list[1], (NTAB, TAPS), TAPS ** -0.5, 1.5, (), jnp.float32)
    range_shift = touch_ends(jax.random.randint(key_list[2], (R,), 0 - MAXSHIFT, MAXSHIFT + 1), jax.random.fold_in(key_list[2], 1), 0 - MAXSHIFT, MAXSHIFT).astype(jnp.int32)
    tap_index = touch_ends(jax.random.randint(key_list[3], (R,), 0, NTAB), jax.random.fold_in(key_list[3], 1), 0, NTAB - 1).astype(jnp.int32)
    ref_channel = touch_ends(jax.random.randint(key_list[4], (N_AZ,), 0, CHAN), jax.random.fold_in(key_list[4], 1), 0, CHAN - 1).astype(jnp.int32)
    return dict(signal=signal, tap_table=tap_table, range_shift=range_shift, tap_index=tap_index, ref_channel=ref_channel)


def spectrum_of(channel_data):
    samples = lax.complex(channel_data[0].astype(jnp.float32), channel_data[1].astype(jnp.float32))
    return jnp.fft.fft(samples, axis=-1) / math.sqrt(samples.shape[-1])

def reference(signal, tap_table, range_shift, tap_index, ref_channel):
    pulse_total = signal.shape[2]
    block_len = pulse_total // ref_channel.shape[0]
    per_pulse = jnp.repeat(ref_channel.astype(jnp.int32), block_len)
    pulse_ids = jnp.arange(pulse_total, dtype=jnp.int32)
    chosen = jnp.stack([signal[per_pulse, 0, pulse_ids, :], signal[per_pulse, 1, pulse_ids, :]])
    ref_spec = spectrum_of(chosen)
    magnitude = jnp.real(ref_spec) ** 2 + jnp.imag(ref_spec) ** 2
    weighting = jnp.conj(ref_spec) * lax.rsqrt(jnp.maximum(magnitude, 1.0))
    weight_real = jnp.real(weighting).astype(jnp.bfloat16)
    weight_imag = jnp.imag(weighting).astype(jnp.bfloat16)
    weight_real, weight_imag = lax.optimization_barrier((weight_real, weight_imag))
    weighting = lax.complex(weight_real.astype(jnp.float32), weight_imag.astype(jnp.float32))
    tap_rows = tap_table[tap_index]
    lag_count = range_shift.shape[0]
    positions = jnp.arange(lag_count, dtype=jnp.int32) + HALO + range_shift.astype(jnp.int32) - TAPS // 2

    def per_channel(channel_data):
        product = spectrum_of(channel_data) * weighting
        lagged = jnp.fft.ifft(product, axis=-1) * math.sqrt(product.shape[-1])
        lagged = lagged[:, GUARD:GUARD + lag_count]
        real_low = jnp.real(lagged).astype(jnp.bfloat16)
        imag_low = jnp.imag(lagged).astype(jnp.bfloat16)
        real_low, imag_low = lax.optimization_barrier((real_low, imag_low))
        compressed = lax.complex(real_low.astype(jnp.float32), imag_low.astype(jnp.float32))
        padded = jnp.pad(compressed, ((0, 0), (HALO, HALO)))
        aligned = jnp.zeros_like(compressed)
        for tap_pos in range(TAPS):
            aligned = aligned + tap_rows[:, tap_pos] * jnp.take(padded, positions + tap_pos, axis=1)
        doppler_map = jnp.fft.fft(aligned, axis=0) / math.sqrt(aligned.shape[0])
        return jnp.stack([jnp.real(doppler_map), jnp.imag(doppler_map)]).astype(jnp.float32)
    return lax.map(per_channel, signal)
```

```python
import functools
import math

import jax
import jax.numpy as jnp
import numpy as np
from jax import lax
from jax.experimental import pallas as pl
from jax.experimental.pallas import tpu as pltpu
from jax.sharding import PartitionSpec as P

TAIL = 128
GUARD = 16
HALO = 16
MESH = pl.DeviceIdType.MESH


def complex_block(table, left):
    top, low = (-table.imag, table.imag) if left else (table.imag, -table.imag)
    return np.block([[table.real, top], [low, table.real]])


def tables(lead, lags, pulses, pul_dev):
    total = lead * TAIL
    lead_idx, tail_idx = np.arange(lead), np.arange(TAIL)
    rows = lags // TAIL + 1
    fwd_lead = complex_block(np.exp(-2j * np.pi * np.outer(lead_idx, lead_idx) / lead), True)
    fwd_tail = complex_block(np.exp(-2j * np.pi * np.outer(tail_idx, tail_idx) / TAIL), False)
    inv_tail = complex_block(np.exp(2j * np.pi * np.outer(tail_idx, tail_idx) / TAIL), False)
    inv_lead = complex_block(np.exp(2j * np.pi * np.outer(np.arange(rows), lead_idx) / lead), True)
    inv_lead = inv_lead.reshape(2, rows, -1).transpose(1, 0, 2).reshape(2 * rows, -1)
    twist = np.exp(-2j * np.pi * np.outer(lead_idx, tail_idx) / total) / math.sqrt(total)
    doppler = complex_block(np.exp(-2j * np.pi * np.outer(np.arange(pulses), np.arange(pulses)) / pulses), True)
    doppler = doppler.reshape(2 * pulses, 2, pulses).transpose(0, 2, 1).reshape(2 * pulses, 2 * pulses)
    low = [item.astype(jnp.bfloat16) for item in (fwd_lead, fwd_tail, inv_tail, inv_lead, doppler)]
    return low, np.stack([twist.real, twist.imag]).astype(np.float32)


def kernel(
    chan_count, az_count, sig, taps, shift, index, source, fwd_lead, fwd_tail, inv_tail, inv_lead, doppler, twist,
    out, quarter, spec, filt, packed, comp, framed, send_a, recv_a, send_b, recv_b, send_c, recv_c,
):
    me_chan, me_az = lax.axis_index("chan"), lax.axis_index("az")
    pul_dev = sig.shape[0]
    lead = sig.shape[1] // 2
    part = pul_dev // chan_count
    slab = shift.shape[1]
    rows = packed.shape[0]
    pulses = az_count * pul_dev

    barrier = pltpu.get_barrier_semaphore()
    for step in range(1, chan_count):
        pl.semaphore_signal(
            barrier, inc=1, device_id={"chan": lax.rem(me_chan + step, chan_count)}, device_id_type=MESH
        )
    for step in range(1, az_count):
        pl.semaphore_signal(barrier, inc=1, device_id={"az": lax.rem(me_az + step, az_count)}, device_id_type=MESH)
    pl.semaphore_wait(barrier, chan_count + az_count - 2)

    first = []
    for step in [*range(2, chan_count), 1]:
        to = lax.rem(me_chan + step, chan_count)
        first.append(
            pltpu.make_async_remote_copy(
                src_ref=sig.at[pl.ds(to * part, part)],
                dst_ref=quarter.at[me_chan],
                send_sem=send_a.at[step],
                recv_sem=recv_a.at[step],
                device_id={"chan": to},
                device_id_type=MESH,
            )
        )
        first[-1].start()
    quarter[me_chan] = sig[pl.ds(me_chan * part, part)]

    twist_real, twist_imag = twist[0], twist[1]

    def forward(blocks):
        data = jnp.concatenate(blocks, axis=1) if len(blocks) > 1 else blocks[0]
        step = jnp.dot(fwd_lead[...], data, preferred_element_type=jnp.float32)
        turned = []
        for pos in range(len(blocks)):
            real = step[:lead, pos * TAIL : (pos + 1) * TAIL]
            imag = step[lead:, pos * TAIL : (pos + 1) * TAIL]
            turned.append(
                jnp.concatenate(
                    [real * twist_real - imag * twist_imag, real * twist_imag + imag * twist_real], axis=1
                ).astype(jnp.bfloat16)
            )
        turned = jnp.concatenate(turned, axis=0) if len(turned) > 1 else turned[0]
        return jnp.dot(turned, fwd_tail[...], preferred_element_type=jnp.float32)

    spec[...] = forward([sig[pos] for pos in range(pul_dev)]).reshape(spec.shape)

    entries = taps.shape[0]
    chooser = (lax.broadcasted_iota(jnp.int32, (entries, slab), 0) == index[...]).astype(jnp.bfloat16)
    tap_rows = lax.dot_general(
        taps[...].astype(jnp.bfloat16), chooser, (((0,), (0,)), ((), ())), preferred_element_type=jnp.float32
    )
    tap_count = tap_rows.shape[0]
    reach = slab + TAIL
    offset = (
        lax.broadcasted_iota(jnp.int32, (reach, slab), 0)
        - lax.broadcasted_iota(jnp.int32, (reach, slab), 1)
        - (HALO - tap_count // 2)
        - shift[...]
    )
    band = jnp.zeros((reach, slab), jnp.float32)
    for tap in range(tap_count):
        band = jnp.where(offset == tap, tap_rows[tap : tap + 1, :], band)
    band = band.astype(jnp.bfloat16)

    for copy in first:
        copy.wait()
    chosen = quarter[source[0]]
    ref = forward([chosen[pos] for pos in range(part)])
    real, imag = ref[:, :TAIL], ref[:, TAIL:]
    inverse = lax.rsqrt(jnp.maximum(real * real + imag * imag, 1.0))
    filt[me_chan] = jnp.concatenate([real * inverse, -imag * inverse], axis=1).astype(jnp.bfloat16)

    second = []
    for step in [*range(2, chan_count), 1]:
        to = lax.rem(me_chan + step, chan_count)
        second.append(
            pltpu.make_async_remote_copy(
                src_ref=filt.at[me_chan],
                dst_ref=filt.at[me_chan],
                send_sem=send_b.at[step],
                recv_sem=recv_b.at[step],
                device_id={"chan": to},
                device_id_type=MESH,
            )
        )
        second[-1].start()
    for copy in second:
        copy.wait()

    weight = filt[...].reshape(pul_dev * lead, 2 * TAIL).astype(jnp.float32)
    own = spec[...].reshape(pul_dev * lead, 2 * TAIL)
    spec_real, spec_imag = own[:, :TAIL], own[:, TAIL:]
    filt_real, filt_imag = weight[:, :TAIL], weight[:, TAIL:]
    product = jnp.concatenate(
        [spec_real * filt_real - spec_imag * filt_imag, spec_real * filt_imag + spec_imag * filt_real], axis=1
    ).astype(jnp.bfloat16)
    lagged = jnp.dot(product, inv_tail[...], preferred_element_type=jnp.float32)
    columns = []
    for pos in range(pul_dev):
        real = lagged[pos * lead : (pos + 1) * lead, :TAIL]
        imag = lagged[pos * lead : (pos + 1) * lead, TAIL:]
        columns.append(
            jnp.concatenate(
                [real * twist_real + imag * twist_imag, imag * twist_real - real * twist_imag], axis=0
            ).astype(jnp.bfloat16)
        )
    lags = jnp.dot(inv_lead[...], jnp.concatenate(columns, axis=1), preferred_element_type=jnp.float32)
    for pos in range(pul_dev):
        block = lags[:, pos * TAIL : (pos + 1) * TAIL]
        for row in range(rows):
            packed[row, 2 * pos : 2 * pos + 2, :] = block[2 * row : 2 * row + 2, :]
    when = lax.broadcasted_iota(jnp.int32, packed.shape, 0) * TAIL + lax.broadcasted_iota(jnp.int32, packed.shape, 2)
    inside = (when >= GUARD) & (when < GUARD + slab * az_count)
    comp[...] = jnp.where(inside, packed[...], 0.0).astype(jnp.bfloat16)

    third = []
    for step in range(1, az_count):
        to = lax.rem(me_az + step, az_count)
        third.append(
            pltpu.make_async_remote_copy(
                src_ref=comp.at[pl.ds(to, 2)],
                dst_ref=framed.at[me_az],
                send_sem=send_c.at[step],
                recv_sem=recv_c.at[step],
                device_id={"az": to},
                device_id_type=MESH,
            )
        )
        third[-1].start()
    framed[me_az] = comp[pl.ds(me_az, 2)]
    for copy in third:
        copy.wait()

    main = framed[:, 0].reshape(2 * pulses, TAIL)
    after = framed[:, 1].reshape(2 * pulses, TAIL)
    aligned = jnp.dot(jnp.concatenate([main, after], axis=1), band, preferred_element_type=jnp.float32)
    picture = jnp.dot(doppler[...], aligned.astype(jnp.bfloat16), preferred_element_type=jnp.float32)
    out[...] = picture * (1.0 / math.sqrt(pulses))


def shards(signal, tap_table, range_shift, tap_index, ref_channel):
    chan_count, az_count = lax.axis_size("chan"), lax.axis_size("az")
    pul_dev, samples = signal.shape[2], signal.shape[3]
    lead = samples // TAIL
    slab = range_shift.shape[0]
    part = pul_dev // chan_count
    pulses = pul_dev * az_count
    lags = slab * az_count
    rows = lags // TAIL + 1
    low, twist = tables(lead, lags, pulses, pul_dev)
    sig = signal[0].reshape(2, pul_dev, lead, TAIL).transpose(1, 0, 2, 3).reshape(pul_dev, 2 * lead, TAIL)
    vmem = pl.BlockSpec(memory_space=pltpu.VMEM)
    dma = pltpu.SemaphoreType.DMA
    picture = pl.pallas_call(
        functools.partial(kernel, chan_count, az_count),
        out_shape=jax.ShapeDtypeStruct((2 * pulses, slab), jnp.float32),
        in_specs=[vmem] * 4 + [pl.BlockSpec(memory_space=pltpu.SMEM)] + [vmem] * 6,
        out_specs=vmem,
        scratch_shapes=[
            pltpu.VMEM((chan_count, part, 2 * lead, TAIL), jnp.bfloat16),
            pltpu.VMEM((pul_dev, lead, 2 * TAIL), jnp.float32),
            pltpu.VMEM((chan_count, part * lead, 2 * TAIL), jnp.bfloat16),
            pltpu.VMEM((rows, 2 * pul_dev, TAIL), jnp.float32),
            pltpu.VMEM((rows, 2 * pul_dev, TAIL), jnp.bfloat16),
            pltpu.VMEM((az_count, 2, 2 * pul_dev, TAIL), jnp.bfloat16),
            dma((chan_count,)),
            dma((chan_count,)),
            dma((chan_count,)),
            dma((chan_count,)),
            dma((az_count,)),
            dma((az_count,)),
        ],
        compiler_params=pltpu.CompilerParams(collective_id=0, has_side_effects=True, vmem_limit_bytes=48 * 2**20),
    )(
        sig,
        tap_table,
        range_shift.reshape(1, slab),
        tap_index.reshape(1, slab),
        ref_channel,
        *[jnp.asarray(item) for item in low],
        jnp.asarray(twist),
    )
    return picture.reshape(1, 2, pulses, slab)


def solution(mesh):
    return jax.shard_map(
        shards,
        mesh=mesh,
        in_specs=(P("chan", None, "az", None), P(), P("az"), P("az"), P("az")),
        out_specs=P("chan", None, None, "az"),
        check_vma=False,
    )
```

```python
import functools
import math

import jax
import jax.numpy as jnp
import numpy as np
from jax import lax
from jax.experimental import pallas as pl
from jax.experimental.pallas import tpu as pltpu
from jax.sharding import PartitionSpec as P

TAIL = 128
GUARD = 16
HALO = 16
MESH = pl.DeviceIdType.MESH


def complex_block(table, left):
    top, low = (-table.imag, table.imag) if left else (table.imag, -table.imag)
    return np.block([[table.real, top], [low, table.real]])


def tables(lead, lags, az_count, pul_dev, chunks, groups):
    total = lead * TAIL
    pulses = az_count * pul_dev
    lead_idx, tail_idx = np.arange(lead), np.arange(TAIL)
    rows = lags // TAIL + 1
    fwd_lead = complex_block(np.exp(-2j * np.pi * np.outer(lead_idx, lead_idx) / lead), True)
    fwd_tail = complex_block(np.exp(-2j * np.pi * np.outer(tail_idx, tail_idx) / TAIL), False)
    inv_tail = complex_block(np.exp(2j * np.pi * np.outer(tail_idx, tail_idx) / TAIL), False)
    inv_lead = complex_block(np.exp(2j * np.pi * np.outer(np.arange(rows), lead_idx) / lead), True)
    inv_lead = inv_lead.reshape(2, rows, -1).transpose(1, 0, 2).reshape(2 * rows, -1)
    twist = np.exp(-2j * np.pi * np.outer(lead_idx, tail_idx) / total) / math.sqrt(total)
    doppler = complex_block(np.exp(-2j * np.pi * np.outer(np.arange(pulses), np.arange(pulses)) / pulses), True)
    doppler = doppler.reshape(2 * pulses, 2, az_count, 2, groups, -1).transpose(0, 4, 2, 3, 5, 1)
    low = [fwd_lead, fwd_tail, inv_tail, inv_lead, doppler.reshape(2 * pulses, 2 * pulses)]
    return [item.astype(jnp.bfloat16) for item in low], np.stack([twist.real, twist.imag]).astype(np.float32)


def kernel(
    chan_count, az_count, chunks, groups, sig, taps, shift, index, source, fwd_lead, fwd_tail, inv_tail, inv_lead,
    doppler, twist, out, mate, cand, spec, filt, packed, comp, framed, send_a, recv_a, send_b, recv_b, send_c, recv_c,
    send_d, recv_d,
):
    me_chan, me_az = lax.axis_index("chan"), lax.axis_index("az")
    pul_dev, lead = sig.shape[1], sig.shape[2]
    half = pul_dev // 2
    part = half // chunks
    chips = chan_count // 2
    side, chip = lax.rem(me_chan, 2), me_chan // 2
    other = 1 - side
    sibling = {"chan": chip * 2 + other}
    slab = shift.shape[1]
    rows = comp.shape[1]
    per_group = chunks // groups

    def across(step):
        return {"chan": lax.rem(chip + step, chips) * 2 + side}

    def along(step):
        return lax.rem(me_az + step, az_count)

    barrier = pltpu.get_barrier_semaphore()
    peers = [sibling, *[across(step) for step in range(1, chips)], *[{"az": along(step)} for step in range(1, az_count)]]
    for peer in peers:
        pl.semaphore_signal(barrier, inc=1, device_id=peer, device_id_type=MESH)
    pl.semaphore_wait(barrier, len(peers))

    started = []

    def send(src, dst, send_sem, recv_sem, peer):
        copy = pltpu.make_async_remote_copy(
            src_ref=src, dst_ref=dst, send_sem=send_sem, recv_sem=recv_sem, device_id=peer, device_id_type=MESH
        )
        copy.start()
        started.append(copy)
        return copy

    first = [
        send(sig.at[:, pl.ds(other * half + pos * part, part)], mate.at[pos], send_a.at[pos], recv_a.at[pos], sibling)
        for pos in range(chunks)
    ]
    chosen_side, chosen_chip = lax.rem(source[0], 2), source[0] // 2
    second = []
    for pos in range(chunks):
        first[pos].wait_recv()
        mine = sig[:, pl.ds(side * half + pos * part, part)]
        cand[chip, pos] = jnp.where(chosen_side == side, mine, mate[pos])
        second.append(
            [
                send(
                    cand.at[chip, pos], cand.at[chip, pos], send_b.at[step, pos], recv_b.at[step, pos], across(step)
                )
                for step in range(1, chips)
            ]
        )

    twist_real, twist_imag = twist[0], twist[1]

    def forward(blocks):
        step = jnp.dot(fwd_lead[...], jnp.concatenate(blocks, axis=1), preferred_element_type=jnp.float32)
        turned = []
        for pos in range(len(blocks)):
            real = step[:lead, pos * TAIL : (pos + 1) * TAIL]
            imag = step[lead:, pos * TAIL : (pos + 1) * TAIL]
            turned.append(
                jnp.concatenate(
                    [real * twist_real - imag * twist_imag, real * twist_imag + imag * twist_real], axis=1
                ).astype(jnp.bfloat16)
            )
        return jnp.dot(jnp.concatenate(turned, axis=0), fwd_tail[...], preferred_element_type=jnp.float32)

    def stacked(block):
        return [jnp.concatenate([block[0, pos], block[1, pos]], axis=0) for pos in range(block.shape[1])]

    spec[...] = forward(stacked(sig[...])).reshape(spec.shape)

    entries = taps.shape[0]
    chooser = (lax.broadcasted_iota(jnp.int32, (entries, slab), 0) == index[...]).astype(jnp.bfloat16)
    tap_rows = lax.dot_general(
        taps[...].astype(jnp.bfloat16), chooser, (((0,), (0,)), ((), ())), preferred_element_type=jnp.float32
    )
    tap_count = tap_rows.shape[0]
    reach = slab + TAIL
    offset = (
        lax.broadcasted_iota(jnp.int32, (reach, slab), 0)
        - lax.broadcasted_iota(jnp.int32, (reach, slab), 1)
        - (HALO - tap_count // 2)
        - shift[...]
    )
    band = jnp.zeros((reach, slab), jnp.float32)
    for tap in range(tap_count):
        band = jnp.where(offset == tap, tap_rows[tap : tap + 1, :], band)
    band = band.astype(jnp.bfloat16)

    def backward(which, pos):
        weight = filt[which, pos].astype(jnp.float32)
        own = spec[which, pos]
        spec_real, spec_imag = own[:, :TAIL], own[:, TAIL:]
        filt_real, filt_imag = weight[:, :TAIL], weight[:, TAIL:]
        product = jnp.concatenate(
            [spec_real * filt_real - spec_imag * filt_imag, spec_real * filt_imag + spec_imag * filt_real], axis=1
        ).astype(jnp.bfloat16)
        lagged = jnp.dot(product, inv_tail[...], preferred_element_type=jnp.float32)
        columns = []
        for step in range(part):
            real = lagged[step * lead : (step + 1) * lead, :TAIL]
            imag = lagged[step * lead : (step + 1) * lead, TAIL:]
            columns.append(
                jnp.concatenate(
                    [real * twist_real + imag * twist_imag, imag * twist_real - real * twist_imag], axis=0
                ).astype(jnp.bfloat16)
            )
        lags = jnp.dot(inv_lead[...], jnp.concatenate(columns, axis=1), preferred_element_type=jnp.float32)
        group, place = pos // per_group, pos % per_group
        for step in range(part):
            start = 2 * (place * part + step)
            for row in range(rows):
                packed[which, group, row, start : start + 2, :] = lags[
                    2 * row : 2 * row + 2, step * TAIL : (step + 1) * TAIL
                ]

    fourth = []
    for pos in range(chunks):
        for copy in second[pos]:
            copy.wait_recv()
        chosen = cand[0, pos]
        for place in range(1, chips):
            chosen = jnp.where(chosen_chip == place, cand[place, pos], chosen)
        ref = forward(stacked(chosen))
        real, imag = ref[:, :TAIL], ref[:, TAIL:]
        inverse = lax.rsqrt(jnp.maximum(real * real + imag * imag, 1.0))
        filt[side, pos] = jnp.concatenate([real * inverse, -imag * inverse], axis=1).astype(jnp.bfloat16)
        third = send(filt.at[side, pos], filt.at[side, pos], send_c.at[pos], recv_c.at[pos], sibling)
        backward(side, pos)
        third.wait_recv()
        backward(other, pos)
        if pos % per_group == per_group - 1:
            group = pos // per_group
            lags = jnp.concatenate([packed[0, group], packed[1, group]], axis=1)
            when = lax.broadcasted_iota(jnp.int32, lags.shape, 0) * TAIL + lax.broadcasted_iota(
                jnp.int32, lags.shape, 2
            )
            inside = (when >= GUARD) & (when < GUARD + slab * az_count)
            comp[group] = jnp.where(inside, lags, 0.0).astype(jnp.bfloat16)
            fourth.append(
                [
                    send(
                        comp.at[group, pl.ds(along(step), 2)],
                        framed.at[group, me_az],
                        send_d.at[group, step],
                        recv_d.at[group, step],
                        {"az": along(step)},
                    )
                    for step in range(1, az_count)
                ]
            )
            framed[group, me_az] = comp[group, pl.ds(me_az, 2)]

    aligned = []
    for group in range(groups):
        for copy in fourth[group]:
            copy.wait_recv()
        main = framed[group, :, 0].reshape(az_count * comp.shape[2], TAIL)
        after = framed[group, :, 1].reshape(az_count * comp.shape[2], TAIL)
        aligned.append(
            jnp.dot(jnp.concatenate([main, after], axis=1), band, preferred_element_type=jnp.float32).astype(
                jnp.bfloat16
            )
        )
    picture = jnp.dot(doppler[...], jnp.concatenate(aligned, axis=0), preferred_element_type=jnp.float32)
    out[...] = picture * (1.0 / math.sqrt(az_count * pul_dev))
    for copy in started:
        copy.wait_send()


def shards(signal, tap_table, range_shift, tap_index, ref_channel):
    chan_count, az_count = lax.axis_size("chan"), lax.axis_size("az")
    pul_dev, samples = signal.shape[2], signal.shape[3]
    lead = samples // TAIL
    slab = range_shift.shape[0]
    chips = chan_count // 2
    chunks, groups = pul_dev // 4, 2
    part = pul_dev // 2 // chunks
    pulses = pul_dev * az_count
    lags = slab * az_count
    rows = lags // TAIL + 1
    low, twist = tables(lead, lags, az_count, pul_dev, chunks, groups)
    sig = signal[0].reshape(2, pul_dev, lead, TAIL)
    vmem = pl.BlockSpec(memory_space=pltpu.VMEM)
    dma = pltpu.SemaphoreType.DMA
    picture = pl.pallas_call(
        functools.partial(kernel, chan_count, az_count, chunks, groups),
        out_shape=jax.ShapeDtypeStruct((2 * pulses, slab), jnp.float32),
        in_specs=[vmem] * 4 + [pl.BlockSpec(memory_space=pltpu.SMEM)] + [vmem] * 6,
        out_specs=vmem,
        scratch_shapes=[
            pltpu.VMEM((chunks, 2, part, lead, TAIL), jnp.bfloat16),
            pltpu.VMEM((chips, chunks, 2, part, lead, TAIL), jnp.bfloat16),
            pltpu.VMEM((2, chunks, part * lead, 2 * TAIL), jnp.float32),
            pltpu.VMEM((2, chunks, part * lead, 2 * TAIL), jnp.bfloat16),
            pltpu.VMEM((2, groups, rows, pul_dev // groups, TAIL), jnp.float32),
            pltpu.VMEM((groups, rows, 2 * pul_dev // groups, TAIL), jnp.bfloat16),
            pltpu.VMEM((groups, az_count, 2, 2 * pul_dev // groups, TAIL), jnp.bfloat16),
            dma((chunks,)),
            dma((chunks,)),
            dma((chips, chunks)),
            dma((chips, chunks)),
            dma((chunks,)),
            dma((chunks,)),
            dma((groups, az_count)),
            dma((groups, az_count)),
        ],
        compiler_params=pltpu.CompilerParams(collective_id=0, has_side_effects=True, vmem_limit_bytes=48 * 2**20),
    )(
        sig,
        tap_table,
        range_shift.reshape(1, slab),
        tap_index.reshape(1, slab),
        ref_channel,
        *[jnp.asarray(item) for item in low],
        jnp.asarray(twist),
    )
    return picture.reshape(1, 2, pulses, slab)


def solution(mesh):
    return jax.shard_map(
        shards,
        mesh=mesh,
        in_specs=(P("chan", None, "az", None), P(), P("az"), P("az"), P("az")),
        out_specs=P("chan", None, None, "az"),
        check_vma=False,
    )
```

```python
import functools
import math

import jax
import jax.numpy as jnp
import numpy as np
from jax import lax
from jax.experimental import pallas as pl
from jax.experimental.pallas import tpu as pltpu
from jax.sharding import PartitionSpec as P

TAIL = 128
GUARD = 16
HALO = 16
MESH = pl.DeviceIdType.MESH


def complex_block(table, left):
    top, low = (-table.imag, table.imag) if left else (table.imag, -table.imag)
    return np.block([[table.real, top], [low, table.real]])


def tables(lead, lags, az_count, pul_dev, chunks, groups):
    total = lead * TAIL
    pulses = az_count * pul_dev
    lead_idx, tail_idx = np.arange(lead), np.arange(TAIL)
    rows = lags // TAIL + 1
    fwd_lead = complex_block(np.exp(-2j * np.pi * np.outer(lead_idx, lead_idx) / lead), True)
    fwd_tail = complex_block(np.exp(-2j * np.pi * np.outer(tail_idx, tail_idx) / TAIL), False)
    inv_tail = complex_block(np.exp(2j * np.pi * np.outer(tail_idx, tail_idx) / TAIL), False)
    inv_lead = complex_block(np.exp(2j * np.pi * np.outer(np.arange(rows), lead_idx) / lead), True)
    inv_lead = inv_lead.reshape(2, rows, -1).transpose(1, 0, 2).reshape(2 * rows, -1)
    twist = np.exp(-2j * np.pi * np.outer(lead_idx, tail_idx) / total) / math.sqrt(total)
    doppler = complex_block(np.exp(-2j * np.pi * np.outer(np.arange(pulses), np.arange(pulses)) / pulses), True)
    doppler = doppler.reshape(2 * pulses, 2, az_count, 2, groups, -1).transpose(0, 4, 2, 3, 5, 1)
    low = [fwd_lead, fwd_tail, inv_tail, inv_lead, doppler.reshape(2 * pulses, 2 * pulses)]
    return [item.astype(jnp.bfloat16) for item in low], np.stack([twist.real, twist.imag]).astype(np.float32)


def kernel(
    chan_count, az_count, chunks, groups, sig, taps, shift, index, source, fwd_lead, fwd_tail, inv_tail, inv_lead,
    doppler, twist, out, mate, cand, spec, filt, packed, comp, framed, send_a, recv_a, send_b, recv_b, send_c, recv_c,
    send_d, recv_d,
):
    me_chan, me_az = lax.axis_index("chan"), lax.axis_index("az")
    pul_dev, lead = sig.shape[1], sig.shape[2]
    half = pul_dev // 2
    part = half // chunks
    chips = chan_count // 2
    side, chip = lax.rem(me_chan, 2), me_chan // 2
    other = 1 - side
    sibling = {"chan": chip * 2 + other}
    slab = shift.shape[1]
    rows = comp.shape[1]
    per_group = chunks // groups

    def across(step):
        return {"chan": lax.rem(chip + step, chips) * 2 + side}

    def along(step):
        return lax.rem(me_az + step, az_count)

    barrier = pltpu.get_barrier_semaphore()
    peers = [sibling, *[across(step) for step in range(1, chips)], *[{"az": along(step)} for step in range(1, az_count)]]
    for peer in peers:
        pl.semaphore_signal(barrier, inc=1, device_id=peer, device_id_type=MESH)

    entries = taps.shape[1]
    chooser = (lax.broadcasted_iota(jnp.int32, (entries, slab), 0) == index[...]).astype(jnp.bfloat16)
    tap_rows = jnp.dot(taps[...].astype(jnp.bfloat16), chooser, preferred_element_type=jnp.float32)
    tap_count = tap_rows.shape[0]
    reach = slab + TAIL
    offset = (
        lax.broadcasted_iota(jnp.int32, (reach, slab), 0)
        - lax.broadcasted_iota(jnp.int32, (reach, slab), 1)
        - (HALO - tap_count // 2)
        - shift[...]
    )
    band = jnp.zeros((reach, slab), jnp.float32)
    for tap in range(tap_count):
        band = jnp.where(offset == tap, tap_rows[tap : tap + 1, :], band)
    band = band.astype(jnp.bfloat16)

    pl.semaphore_wait(barrier, len(peers))

    started = []

    def send(src, dst, send_sem, recv_sem, peer):
        copy = pltpu.make_async_remote_copy(
            src_ref=src, dst_ref=dst, send_sem=send_sem, recv_sem=recv_sem, device_id=peer, device_id_type=MESH
        )
        copy.start()
        started.append(copy)
        return copy

    first = [
        send(sig.at[:, pl.ds(other * half + pos * part, part)], mate.at[pos], send_a.at[pos], recv_a.at[pos], sibling)
        for pos in range(chunks)
    ]
    twist_real, twist_imag = twist[0], twist[1]

    def forward(blocks):
        step = jnp.dot(fwd_lead[...], jnp.concatenate(blocks, axis=1), preferred_element_type=jnp.float32)
        turned = []
        for pos in range(len(blocks)):
            real = step[:lead, pos * TAIL : (pos + 1) * TAIL]
            imag = step[lead:, pos * TAIL : (pos + 1) * TAIL]
            turned.append(
                jnp.concatenate(
                    [real * twist_real - imag * twist_imag, real * twist_imag + imag * twist_real], axis=1
                ).astype(jnp.bfloat16)
            )
        return jnp.dot(jnp.concatenate(turned, axis=0), fwd_tail[...], preferred_element_type=jnp.float32)

    def stacked(block):
        return [jnp.concatenate([block[0, pos], block[1, pos]], axis=0) for pos in range(block.shape[1])]

    early = chunks // 2
    spec[0, :early] = forward(stacked(sig[:, : early * part])).reshape(early, part * lead, 2 * TAIL)

    chosen_side, chosen_chip = lax.rem(source[0], 2), source[0] // 2
    second = []
    for pos in range(chunks):
        first[pos].wait_recv()
        mine = sig[:, pl.ds(side * half + pos * part, part)]
        cand[chip, pos] = jnp.where(chosen_side == side, mine, mate[pos])
        second.append(
            [
                send(
                    cand.at[chip, pos], cand.at[chip, pos], send_b.at[step, pos], recv_b.at[step, pos], across(step)
                )
                for step in range(1, chips)
            ]
        )

    spec[0, early:] = forward(stacked(sig[:, early * part : half])).reshape(chunks - early, part * lead, 2 * TAIL)
    spec[1] = forward(stacked(sig[:, half:])).reshape(chunks, part * lead, 2 * TAIL)

    def backward(which, pos):
        weight = filt[which, pos].astype(jnp.float32)
        own = spec[which, pos]
        spec_real, spec_imag = own[:, :TAIL], own[:, TAIL:]
        filt_real, filt_imag = weight[:, :TAIL], weight[:, TAIL:]
        product = jnp.concatenate(
            [spec_real * filt_real - spec_imag * filt_imag, spec_real * filt_imag + spec_imag * filt_real], axis=1
        ).astype(jnp.bfloat16)
        lagged = jnp.dot(product, inv_tail[...], preferred_element_type=jnp.float32)
        columns = []
        for step in range(part):
            real = lagged[step * lead : (step + 1) * lead, :TAIL]
            imag = lagged[step * lead : (step + 1) * lead, TAIL:]
            columns.append(
                jnp.concatenate(
                    [real * twist_real + imag * twist_imag, imag * twist_real - real * twist_imag], axis=0
                ).astype(jnp.bfloat16)
            )
        lags = jnp.dot(inv_lead[...], jnp.concatenate(columns, axis=1), preferred_element_type=jnp.float32)
        group, place = pos // per_group, pos % per_group
        for step in range(part):
            start = 2 * (place * part + step)
            for row in range(rows):
                packed[which, group, row, start : start + 2, :] = lags[
                    2 * row : 2 * row + 2, step * TAIL : (step + 1) * TAIL
                ]

    fourth = []

    def finish(pos):
        third[pos].wait_recv()
        backward(other, pos)
        if pos % per_group == per_group - 1:
            group = pos // per_group
            lags = jnp.concatenate([packed[0, group], packed[1, group]], axis=1)
            when = lax.broadcasted_iota(jnp.int32, lags.shape, 0) * TAIL + lax.broadcasted_iota(
                jnp.int32, lags.shape, 2
            )
            inside = (when >= GUARD) & (when < GUARD + slab * az_count)
            comp[group] = jnp.where(inside, lags, 0.0).astype(jnp.bfloat16)
            fourth.append(
                [
                    send(
                        comp.at[group, pl.ds(along(step), 2)],
                        framed.at[group, me_az],
                        send_d.at[group, step],
                        recv_d.at[group, step],
                        {"az": along(step)},
                    )
                    for step in range(1, az_count)
                ]
            )
            framed[group, me_az] = comp[group, pl.ds(me_az, 2)]

    third = []
    for pos in range(chunks):
        for copy in second[pos]:
            copy.wait_recv()
        chosen = cand[0, pos]
        for place in range(1, chips):
            chosen = jnp.where(chosen_chip == place, cand[place, pos], chosen)
        ref = forward(stacked(chosen))
        real, imag = ref[:, :TAIL], ref[:, TAIL:]
        inverse = lax.rsqrt(jnp.maximum(real * real + imag * imag, 1.0))
        filt[side, pos] = jnp.concatenate([real * inverse, -imag * inverse], axis=1).astype(jnp.bfloat16)
        third.append(send(filt.at[side, pos], filt.at[side, pos], send_c.at[pos], recv_c.at[pos], sibling))
        if pos:
            finish(pos - 1)
        backward(side, pos)
    finish(chunks - 1)

    aligned = []
    for group in range(groups):
        for copy in fourth[group]:
            copy.wait_recv()
        main = framed[group, :, 0].reshape(az_count * comp.shape[2], TAIL)
        after = framed[group, :, 1].reshape(az_count * comp.shape[2], TAIL)
        aligned.append(
            jnp.dot(jnp.concatenate([main, after], axis=1), band, preferred_element_type=jnp.float32).astype(
                jnp.bfloat16
            )
        )
    picture = jnp.dot(doppler[...], jnp.concatenate(aligned, axis=0), preferred_element_type=jnp.float32)
    out[...] = picture * (1.0 / math.sqrt(az_count * pul_dev))
    for copy in started:
        copy.wait_send()


def shards(signal, tap_table, range_shift, tap_index, ref_channel):
    chan_count, az_count = lax.axis_size("chan"), lax.axis_size("az")
    pul_dev, samples = signal.shape[2], signal.shape[3]
    lead = samples // TAIL
    slab = range_shift.shape[0]
    chips = chan_count // 2
    chunks, groups = pul_dev // 4, 2
    part = pul_dev // 2 // chunks
    pulses = pul_dev * az_count
    lags = slab * az_count
    rows = lags // TAIL + 1
    low, twist = tables(lead, lags, az_count, pul_dev, chunks, groups)
    sig = signal[0].reshape(2, pul_dev, lead, TAIL)
    vmem = pl.BlockSpec(memory_space=pltpu.VMEM)
    dma = pltpu.SemaphoreType.DMA
    picture = pl.pallas_call(
        functools.partial(kernel, chan_count, az_count, chunks, groups),
        out_shape=jax.ShapeDtypeStruct((2 * pulses, slab), jnp.float32),
        in_specs=[vmem] * 4 + [pl.BlockSpec(memory_space=pltpu.SMEM)] + [vmem] * 6,
        out_specs=vmem,
        scratch_shapes=[
            pltpu.VMEM((chunks, 2, part, lead, TAIL), jnp.bfloat16),
            pltpu.VMEM((chips, chunks, 2, part, lead, TAIL), jnp.bfloat16),
            pltpu.VMEM((2, chunks, part * lead, 2 * TAIL), jnp.float32),
            pltpu.VMEM((2, chunks, part * lead, 2 * TAIL), jnp.bfloat16),
            pltpu.VMEM((2, groups, rows, pul_dev // groups, TAIL), jnp.float32),
            pltpu.VMEM((groups, rows, 2 * pul_dev // groups, TAIL), jnp.bfloat16),
            pltpu.VMEM((groups, az_count, 2, 2 * pul_dev // groups, TAIL), jnp.bfloat16),
            dma((chunks,)),
            dma((chunks,)),
            dma((chips, chunks)),
            dma((chips, chunks)),
            dma((chunks,)),
            dma((chunks,)),
            dma((groups, az_count)),
            dma((groups, az_count)),
        ],
        compiler_params=pltpu.CompilerParams(collective_id=0, has_side_effects=True, vmem_limit_bytes=48 * 2**20),
    )(
        sig,
        tap_table.T,
        range_shift.reshape(1, slab),
        tap_index.reshape(1, slab),
        ref_channel,
        *[jnp.asarray(item) for item in low],
        jnp.asarray(twist),
    )
    return picture.reshape(1, 2, pulses, slab)


def solution(mesh):
    return jax.shard_map(
        shards,
        mesh=mesh,
        in_specs=(P("chan", None, "az", None), P(), P("az"), P("az"), P("az")),
        out_specs=P("chan", None, None, "az"),
        check_vma=False,
    )
```
